32 devices in a mesh: group: 4 (over y, x), dev: 8 (over z, core).
Axes of the slice: x: 2, y: 2, z: 4, core: 2. Of those that a mesh axis runs over, the one named last changes fastest.
Arguments:
- grid_state: bfloat16 [32768, 512], P(('group', 'dev')), may hold values from -6 to 6
- mesh_state: bfloat16 [4096, 512], P(('group', 'dev')), may hold values from -6 to 6
- encode_edge: bfloat16 [512, 512], replicated, may hold values from -0.25 to 0.25
- encode_first: bfloat16 [512, 512], replicated, may hold values from -0.25 to 0.25
- encode_second: bfloat16 [512, 512], replicated, may hold values from -0.25 to 0.25
- process_edge: bfloat16 [512, 512], replicated, may hold values from -0.25 to 0.25
- process_first: bfloat16 [512, 512], replicated, may hold values from -0.25 to 0.25
- process_second: bfloat16 [512, 512], replicated, may hold values from -0.25 to 0.25
- decode_edge: bfloat16 [512, 512], replicated, may hold values from -0.25 to 0.25
- decode_first: bfloat16 [512, 512], replicated, may hold values from -0.25 to 0.25
- decode_second: bfloat16 [512, 512], replicated, may hold values from -0.25 to 0.25
- encode_near: bfloat16 [3, 4096, 1024], P(None, ('group', 'dev')), may hold values from -0.09375 to 0.09375
- encode_live: int32 [3, 256], P(None, ('group', 'dev')), may hold values 0 or 1
- encode_far: bfloat16 [2, 4096, 1024], P(None, ('group', 'dev')), may hold values from -0.09375 to 0.09375
- encode_groups: int32 [2, 32], P(None, ('group', 'dev')), may hold values from 0 to 3, as said below
- process_near: bfloat16 [3, 4096, 128], P(None, ('group', 'dev')), may hold values from -0.25 to 0.25
- process_far: bfloat16 [2, 4096, 128], P(None, ('group', 'dev')), may hold values from -0.25 to 0.25
- process_groups: int32 [2, 32], P(None, ('group', 'dev')), may hold values from 0 to 3, as said below
- decode_near: bfloat16 [3, 32768, 128], P(None, ('group', 'dev')), may hold values from -0.3125 to 0.3125
- decode_live: int32 [3, 256], P(None, ('group', 'dev')), may hold values 0 or 1
Outputs:
- grid_next: bfloat16 [32768, 512], P(('group', 'dev'))
- mesh_next: bfloat16 [4096, 512], P(('group', 'dev'))
The draws below stay inside these ranges and needn't reach their ends.
Inputs may be any that keep to these rules, and one draw needn't show every extreme that they name: `encode_groups`: for each device q the 2 entries of column q are distinct regions, none equal to q's own region q // 8. `process_groups`: for each device q the 2 entries of column q are distinct regions, none equal to q's own region q // 8.
All inputs are finite; a program needn't handle non-finite values. No bound on the sum of `encode_live` or of `decode_live` on one device may be relied on, other than what follows from the above.
Results may differ from the reference program's by a relative error of at most 0.013.
Values may be sent and summed in bfloat16 or wider, within the bound.
A program may use at most 64 MiB of HBM per device.

```python
import jax
import jax.numpy as jnp
from jax import lax

D = 512
TILE = 128
GRID_DEV = 1024
LONG = 2
TILES_DEV = 8
GRID_NODES = 32768
MESH_NODES = 4096
N_GROUP = 4
N_DEV = 8
DEVICES = 32


def far_regions(key):
    total_devices = N_GROUP * N_DEV
    scores = jax.random.randint(key, (total_devices, N_GROUP - 1), 0, 1 << 20) * N_GROUP
    scores = scores + jnp.arange(N_GROUP - 1, dtype=jnp.int32)[None, :]
    chosen = jnp.argsort(scores, axis=1, stable=True)[:, :LONG].astype(jnp.int32)
    own_group = jnp.arange(total_devices, dtype=jnp.int32) // N_DEV
    return ((own_group[:, None] + 1 + chosen) % N_GROUP).T.astype(jnp.int32)


def draw_encode_groups(key, part):
    return far_regions(jax.random.fold_in(key, 11))


def draw_process_groups(key, part):
    return far_regions(jax.random.fold_in(key, 23))


def place_ends(result, own_key, least, high):
    place = [jax.random.randint(jax.random.fold_in(own_key, axis), (), 0, length) for axis, length in enumerate(result.shape)]
    main_axis = result.shape.index(max(result.shape))
    next_to = place[:main_axis] + [(place[main_axis] + 1) % result.shape[main_axis]] + place[main_axis + 1:]
    return result.at[tuple(place)].set(least).at[tuple(next_to)].set(high)


def block_levels(own_key, extent, shards, smallest, largest):
    loudness, own = 1.0, jax.random.fold_in(own_key, 6)
    for axis_at, parts in shards:
        draws = jnp.exp(jax.random.uniform(jax.random.fold_in(own, axis_at), (parts,), jnp.float32, smallest / len(shards), largest / len(shards)))
        loudness = loudness * jnp.repeat(draws, extent[axis_at] // parts).reshape([-1 if axis == axis_at else 1 for axis in range(len(extent))])
    return loudness


def normal_values(stream_key, dims, spread, limit, pieces=(), kind=jnp.bfloat16):
    array = jax.random.normal(stream_key, dims, jnp.float32) * spread
    if len(pieces) > 0:
        array = block_levels(stream_key, dims, pieces, -0.22, 0.18) * array
    return jnp.clip(array, min=-limit, max=limit).astype(kind)


def setup_inputs(seed: int = 0) -> dict:
    key_of = jax.random.split(jax.random.key(seed), 21)
    return {
        "grid_state": normal_values(key_of[0], (GRID_NODES, D), 1.0, 6.0, ((0, 32),)),
        "mesh_state": normal_values(key_of[1], (MESH_NODES, D), 1.0, 6.0, ((0, 32),)),
        "encode_edge": normal_values(key_of[2], (D, D), D ** -0.5, 0.25),
        "encode_first": normal_values(key_of[3], (D, D), D ** -0.5, 0.25),
        "encode_second": normal_values(key_of[4], (D, D), D ** -0.5, 0.25),
        "process_edge": normal_values(key_of[5], (D, D), D ** -0.5, 0.25),
        "process_first": normal_values(key_of[6], (D, D), D ** -0.5, 0.25),
        "process_second": normal_values(key_of[7], (D, D), D ** -0.5, 0.25),
        "decode_edge": normal_values(key_of[8], (D, D), D ** -0.5, 0.25),
        "decode_first": normal_values(key_of[9], (D, D), D ** -0.5, 0.25),
        "decode_second": normal_values(key_of[10], (D, D), D ** -0.5, 0.25),
        "encode_near": normal_values(key_of[11], (3, MESH_NODES, GRID_DEV), (4 * GRID_DEV) ** -0.5, 0.09375, ((1, 32),)),
        "encode_live": place_ends((jax.random.randint(key_of[12], (3, TILES_DEV * DEVICES), 0, 3) < 2).astype(jnp.int32), jax.random.fold_in(key_of[12], 1), 0, 1),
        "encode_far": normal_values(key_of[13], (LONG, MESH_NODES, GRID_DEV), (4 * GRID_DEV) ** -0.5, 0.09375, ((1, 32),)),
        "encode_groups": draw_encode_groups(jax.random.fold_in(key_of[20], 71), 0),
        "process_near": normal_values(key_of[15], (3, MESH_NODES, TILE), (5 * TILE) ** -0.5, 0.25, ((1, 32),)),
        "process_far": normal_values(key_of[16], (LONG, MESH_NODES, TILE), (5 * TILE) ** -0.5, 0.25, ((1, 32),)),
        "process_groups": draw_process_groups(jax.random.fold_in(key_of[20], 71), 0),
        "decode_near": normal_values(key_of[18], (3, GRID_NODES, TILE), (3 * TILE) ** -0.5, 0.3125, ((1, 32),)),
        "decode_live": place_ends((jax.random.randint(key_of[19], (3, TILES_DEV * DEVICES), 0, 3) < 2).astype(jnp.int32), jax.random.fold_in(key_of[19], 1), 0, 1),
    }


highest = lax.Precision.HIGHEST

def layer_norm(row_values):
    row_mean = lax.optimization_barrier(jnp.mean(row_values, axis=-1, keepdims=True))
    centred = row_values - row_mean
    variance = lax.optimization_barrier(jnp.mean(centred * centred, axis=-1, keepdims=True))
    return centred * lax.rsqrt(variance + 1e-05)

def node_update(residual_in, summed, weight_in, weight_out):
    normed = layer_norm(summed).astype(jnp.bfloat16)
    hidden = jax.nn.silu(jnp.dot(normed, weight_in, preferred_element_type=jnp.float32)).astype(jnp.bfloat16)
    updated = residual_in.astype(jnp.float32) + jnp.dot(hidden, weight_out, preferred_element_type=jnp.float32)
    return updated.astype(jnp.bfloat16)

def edge_messages(latents, weight):
    return jax.nn.silu(jnp.dot(latents, weight, preferred_element_type=jnp.float32)).astype(jnp.bfloat16)

def shift_blocks(stacked):
    empty = jnp.zeros_like(stacked[:, :1])
    from_below = jnp.concatenate([empty, stacked[:, :-1]], axis=1)
    from_above = jnp.concatenate([stacked[:, 1:], empty], axis=1)
    return (from_below, from_above)

def reference(grid_state, mesh_state, encode_edge, encode_first, encode_second, process_edge, process_first, process_second, decode_edge, decode_first, decode_second, encode_near, encode_live, encode_far, encode_groups, process_near, process_far, process_groups, decode_near, decode_live):
    enc_msg = edge_messages(grid_state, encode_edge).reshape(N_GROUP, N_DEV, GRID_DEV, D)
    live_enc = encode_live.reshape(3, N_GROUP, N_DEV, TILES_DEV).transpose(1, 0, 2, 3)
    near_enc = encode_near.reshape(3, N_GROUP, N_DEV, TILE, GRID_DEV).transpose(1, 0, 2, 3, 4)
    far_enc = encode_far.reshape(LONG, N_GROUP, N_DEV, TILE, GRID_DEV).transpose(1, 0, 2, 3, 4)

    def group_sources(inputs):
        messages, live_flags, near_tiles, far_tiles = inputs
        wide = messages.astype(jnp.float32)
        near_out = []
        for offset in range(3):
            flags = jnp.repeat(live_flags[offset].astype(jnp.float32), TILE, axis=1)
            masked = wide * flags[:, :, None]
            product = jnp.einsum('dtr,drk->dtk', near_tiles[offset].astype(jnp.float32), masked, precision=highest)
            near_out.append(product.astype(jnp.bfloat16))
        far_out = []
        for index in range(LONG):
            product = jnp.einsum('dtr,drk->dtk', far_tiles[index].astype(jnp.float32), wide, precision=highest)
            far_out.append(product.astype(jnp.bfloat16))
        return (jnp.stack(near_out), jnp.stack(far_out))
    near_part, far_part = lax.map(group_sources, (enc_msg, live_enc, near_enc, far_enc))
    near_wide = near_part.astype(jnp.float32)
    from_below, from_above = shift_blocks(near_wide[:, 2])
    above_part = jnp.concatenate([near_wide[:, 0, 1:], jnp.zeros_like(near_wide[:, 0, :1])], axis=1)
    enc_sum = near_wide[:, 1] + from_below + above_part
    groups_enc = encode_groups.reshape(LONG, N_GROUP, N_DEV)
    select_enc = (groups_enc[..., None] == jnp.arange(N_GROUP, dtype=jnp.int32)).astype(jnp.float32)
    enc_sum = enc_sum + jnp.einsum('lgdh,gldtk->hdtk', select_enc, far_part.astype(jnp.float32), precision=highest)
    mesh_mid = node_update(mesh_state, enc_sum.reshape(MESH_NODES, D), encode_first, encode_second)
    proc_msg = edge_messages(mesh_mid, process_edge).reshape(N_GROUP, N_DEV, TILE, D).astype(jnp.float32)
    below_msg, above_msg = shift_blocks(proc_msg)
    near_proc = process_near.reshape(3, N_GROUP, N_DEV, TILE, TILE).astype(jnp.float32)
    proc_sum = jnp.einsum('gdij,gdjk->gdik', near_proc[0], below_msg, precision=highest)
    proc_sum = proc_sum + jnp.einsum('gdij,gdjk->gdik', near_proc[1], proc_msg, precision=highest)
    proc_sum = proc_sum + jnp.einsum('gdij,gdjk->gdik', near_proc[2], above_msg, precision=highest)
    groups_proc = process_groups.reshape(LONG, N_GROUP, N_DEV)
    select_proc = (groups_proc[..., None] == jnp.arange(N_GROUP, dtype=jnp.int32)).astype(jnp.float32)
    picked = jnp.einsum('lgdh,hdjk->lgdjk', select_proc, proc_msg, precision=highest)
    far_proc = process_far.reshape(LONG, N_GROUP, N_DEV, TILE, TILE).astype(jnp.float32)
    proc_sum = proc_sum + jnp.einsum('lgdij,lgdjk->gdik', far_proc, picked, precision=highest)
    mesh_next = node_update(mesh_mid, proc_sum.reshape(MESH_NODES, D), process_first, process_second)
    dec_msg = edge_messages(mesh_next, decode_edge).reshape(N_GROUP, N_DEV, TILE, D)
    dec_below, dec_above = shift_blocks(dec_msg)
    near_dec = decode_near.reshape(3, N_GROUP, N_DEV, GRID_DEV, TILE).transpose(1, 0, 2, 3, 4)
    live_dec = decode_live.reshape(3, N_GROUP, N_DEV, TILES_DEV).transpose(1, 0, 2, 3)
    grid_groups = grid_state.reshape(N_GROUP, N_DEV * GRID_DEV, D)

    def group_decode(inputs):
        below_blk, own_blk, above_blk, near_tiles, live_flags, grid_rows = inputs
        sources = (below_blk, own_blk, above_blk)
        summed = jnp.zeros((N_DEV, GRID_DEV, D), jnp.float32)
        for offset in range(3):
            product = jnp.einsum('dri,dik->drk', near_tiles[offset].astype(jnp.float32), sources[offset].astype(jnp.float32), precision=highest)
            flags = jnp.repeat(live_flags[offset].astype(jnp.float32), TILE, axis=1)
            summed = summed + product * flags[:, :, None]
        return node_update(grid_rows, summed.reshape(N_DEV * GRID_DEV, D), decode_first, decode_second)
    grid_next = lax.map(group_decode, (dec_below, dec_msg, dec_above, near_dec, live_dec, grid_groups))
    return (grid_next.reshape(GRID_NODES, D), mesh_next)
```

```python
import functools

import jax
import jax.numpy as jnp
from jax import lax
from jax.experimental import pallas as pl
from jax.experimental.pallas import tpu as pltpu
from jax.sharding import PartitionSpec as P

BF16 = jnp.bfloat16
F32 = jnp.float32
CHUNKS = 2


def silu(x):
    half = 0.5 * x
    return half + half * jnp.tanh(half)


def mm(a, b):
    return jnp.dot(a, b, preferred_element_type=F32)


def layer_norm(v):
    mean = jnp.mean(v, axis=-1, keepdims=True)
    cent = v - mean
    var = jnp.mean(cent * cent, axis=-1, keepdims=True)
    return cent * lax.rsqrt(var + 1e-05)


def partner(me, r, count):
    if count & (count - 1):
        return lax.rem(me + r, count), lax.rem(me + count - r, count)
    out, bit = me, 1
    while bit < count:
        if r & bit:
            out = out + bit * (1 - 2 * lax.rem(me // bit, 2))
        bit *= 2
    return out, out


def kernel(
    groups,
    devs,
    grid_h, mesh_h, ee_h, e1_h, e2_h, pe_h, p1_h, p2_h, de_h, d1_h, d2_h,
    en_h, el_h, ef_h, eg_h, pn_h, pf_h, pg_h, dn_h, dl_h,
    grid_o, mesh_o,
    gs, ms, wt, inc, el, eg, pn, pf, pg, dn, dl,
    em, fsend, frecv, nsend, nrecv, msend, mfrecv, mnrecv, dsend, dnrecv,
    own_near, proc_inc, dec_own, mesh_out, grid_out,
    load_sem, fs_sem, fr_sem, ns_sem, nr_sem, mfs_sem, mfr_sem, mns_sem, mnr_sem, ds_sem, dr_sem, out_sem,
):
    g = lax.axis_index("group")
    d = lax.axis_index("dev")
    rows, feats = ms.shape
    width = feats // CHUNKS
    far_count = groups - 1
    long_count = pf.shape[0]
    tiles = el.shape[1]
    peers = [partner(g, r, groups) for r in range(1, groups)]
    order = list(reversed(range(far_count)))
    not_first, not_last = d > 0, d < devs - 1
    sides = ((not_first, d - 1), (not_last, d + 1))

    def load(index, src, dst):
        return pltpu.make_async_copy(src, dst, load_sem.at[index])

    loads = [
        load(0, ee_h, wt.at[0]), load(1, grid_h, gs), load(2, eg_h, eg), load(3, ef_h, inc.at[pl.ds(0, long_count)]),
        load(4, el_h, el), load(5, en_h, inc.at[pl.ds(long_count, 3)]),
        load(6, mesh_h, ms), load(7, e1_h, wt.at[1]), load(8, e2_h, wt.at[2]), load(9, pe_h, wt.at[3]),
        load(10, pg_h, pg), load(11, pn_h, pn), load(12, pf_h, pf), load(13, p1_h, wt.at[4]), load(14, p2_h, wt.at[5]),
        load(15, de_h, wt.at[6]), load(16, dl_h, dl), load(17, dn_h, dn), load(18, d1_h, wt.at[7]), load(19, d2_h, wt.at[8]),
    ]
    for copy in loads[:6]:
        copy.start()

    barrier = pltpu.get_barrier_semaphore()
    for to, _ in peers:
        pl.semaphore_signal(barrier, inc=1, device_id=(to, d), device_id_type=pl.DeviceIdType.MESH)
    if groups & (groups - 1):
        for _, source in peers:
            pl.semaphore_signal(barrier, inc=1, device_id=(source, d), device_id_type=pl.DeviceIdType.MESH)
    for there, near in sides:
        @pl.when(there)
        def _():
            pl.semaphore_signal(barrier, inc=1, device_id=(g, near), device_id_type=pl.DeviceIdType.MESH)

    for copy in loads[6:]:
        copy.start()
    for side, (there, _) in enumerate(sides):
        @pl.when(jnp.logical_not(there))
        def _():
            for buf in (nrecv, mnrecv, dnrecv):
                for c in range(CHUNKS):
                    buf[c, side] = jnp.zeros((rows, width), BF16)

    def remote(src, dst, send, recv, to):
        return pltpu.make_async_remote_copy(
            src_ref=src, dst_ref=dst, send_sem=send, recv_sem=recv, device_id=to, device_id_type=pl.DeviceIdType.MESH
        )

    def far_copy(c, i):
        return remote(fsend.at[c, i], frecv.at[c, i], fs_sem.at[c, i], fr_sem.at[c, i], (peers[i][0], d))

    def near_copy(c, s):
        return remote(nsend.at[c, s], nrecv.at[c, 1 - s], ns_sem.at[c, s], nr_sem.at[c, 1 - s], (g, sides[s][1]))

    def near_in(c, s):
        return remote(nsend.at[c, s], nrecv.at[c, s], ns_sem.at[c, s], nr_sem.at[c, s], (g, sides[s][1]))

    def mfar_copy(c, i):
        return remote(msend.at[c], mfrecv.at[c, i], mfs_sem.at[c, i], mfr_sem.at[c, i], (peers[i][0], d))

    def mnear_copy(c, s):
        return remote(msend.at[c], mnrecv.at[c, 1 - s], mns_sem.at[c, s], mnr_sem.at[c, 1 - s], (g, sides[s][1]))

    def mnear_in(c, s):
        return remote(msend.at[c], mnrecv.at[c, s], mns_sem.at[c, s], mnr_sem.at[c, s], (g, sides[s][1]))

    def dec_copy(c, s):
        return remote(dsend.at[c], dnrecv.at[c, 1 - s], ds_sem.at[c, s], dr_sem.at[c, 1 - s], (g, sides[s][1]))

    def dec_in(c, s):
        return remote(dsend.at[c], dnrecv.at[c, s], ds_sem.at[c, s], dr_sem.at[c, s], (g, sides[s][1]))

    def start_side(copy, c):
        for s, (there, _) in enumerate(sides):
            @pl.when(there)
            def _():
                copy(c, s).start()

    def wait_side(copy, c, s):
        @pl.when(sides[s][0])
        def _():
            copy(c, s).wait_recv()

    loads[0].wait()
    loads[1].wait()
    step = 2 * rows
    for c in range(CHUNKS):
        cols = pl.ds(c * width, width)

        def edge(i, carry):
            at = pl.ds(pl.multiple_of(i * step, step), step)
            em[c, at, :] = silu(mm(gs[at, :], wt[0, :, cols])).astype(BF16)
            return carry

        lax.fori_loop(0, gs.shape[0] // step, edge, 0)
        if c == 0:
            for copy in loads[2:4]:
                copy.wait()
        far = [mm(inc[i], em[c]) for i in range(long_count)]
        if c == 0:
            pl.semaphore_wait(
                barrier,
                far_count * (1 if groups & (groups - 1) == 0 else 2) + jnp.where(not_first, 1, 0) + jnp.where(not_last, 1, 0),
            )
        for i in order:
            total = None
            for index in range(long_count):
                flag = jnp.where(eg[index, 0] == peers[i][0], 1.0, 0.0).astype(F32)
                term = far[index] * flag
                total = term if total is None else total + term
            fsend[c, i] = total.astype(BF16)
            far_copy(c, i).start()
        if c == 0:
            for copy in loads[4:6]:
                copy.wait()
            for k in range(3):
                for t in range(tiles):
                    flag = el[k, t].astype(F32).astype(BF16)
                    at = pl.ds(t * rows, rows)
                    inc[long_count + k, :, at] = inc[long_count + k, :, at] * flag
        for s, k in ((0, 0), (1, 2)):
            nsend[c, s] = mm(inc[long_count + k], em[c]).astype(BF16)
        start_side(near_copy, c)
        own_near[:, cols] = mm(inc[long_count + 1], em[c]).astype(BF16)

    for copy in loads[6:18]:
        copy.wait()
    for i in range(far_count):
        total = None
        for index in range(long_count):
            flag = jnp.where(pg[index, 0] == peers[i][1], 1.0, 0.0).astype(F32)
            term = pf[index].astype(F32) * flag
            total = term if total is None else total + term
        proc_inc[i] = total.astype(BF16)
    for k in range(3):
        for t in range(tiles):
            at = pl.ds(t * rows, rows)
            dn[k, at, :] = dn[k, at, :] * dl[k, t].astype(F32).astype(BF16)

    for copy in loads[18:]:
        copy.wait()

    def node_update(residual, summed, first, second):
        hidden = silu(mm(layer_norm(summed).astype(BF16), wt[first])).astype(BF16)
        return (residual.astype(F32) + mm(hidden, wt[second])).astype(BF16)

    parts = []
    for c in range(CHUNKS):
        total = own_near[:, pl.ds(c * width, width)].astype(F32)
        for s in range(2):
            wait_side(near_in, c, s)
            total = total + nrecv[c, s].astype(F32)
        for i in order:
            far_copy(c, i).wait_recv()
            total = total + frecv[c, i].astype(F32)
        parts.append(total)
    mesh_mid = node_update(ms[...], jnp.concatenate(parts, axis=1), 1, 2)

    for c in range(CHUNKS):
        msend[c] = silu(mm(mesh_mid, wt[3, :, pl.ds(c * width, width)])).astype(BF16)
        for i in order:
            mfar_copy(c, i).start()
        start_side(mnear_copy, c)
    parts = []
    for c in range(CHUNKS):
        total = mm(pn[1], msend[c])
        for s in range(2):
            wait_side(mnear_in, c, s)
            total = total + mm(pn[2 * s], mnrecv[c, s])
        for i in order:
            mfar_copy(c, i).wait_recv()
            total = total + mm(proc_inc[i], mfrecv[c, i])
        parts.append(total)
    mesh_next = node_update(mesh_mid, jnp.concatenate(parts, axis=1), 4, 5)
    mesh_out[...] = mesh_next

    for c in range(CHUNKS):
        dsend[c] = silu(mm(mesh_next, wt[6, :, pl.ds(c * width, width)])).astype(BF16)
        start_side(dec_copy, c)
    mesh_copy = pltpu.make_async_copy(mesh_out, mesh_o, out_sem.at[0])
    mesh_copy.start()

    def own_part(i, carry):
        at = pl.ds(pl.multiple_of(i * step, step), step)
        for c in range(CHUNKS):
            dec_own[at, pl.ds(c * width, width)] = mm(dn[1, at, :], dsend[c])
        return carry

    count = gs.shape[0] // step
    lax.fori_loop(0, count, own_part, 0)
    for c in range(CHUNKS):
        for s in range(2):
            wait_side(dec_in, c, s)
    outs = []
    for i in range(count):
        at = pl.ds(i * step, step)
        sums = []
        for c in range(CHUNKS):
            total = dec_own[at, pl.ds(c * width, width)]
            for s in range(2):
                total = total + mm(dn[2 * s, at, :], dnrecv[c, s])
            sums.append(total)
        grid_out[at, :] = node_update(gs[at, :], jnp.concatenate(sums, axis=1), 7, 8)
        copy = pltpu.make_async_copy(grid_out.at[at], grid_o.at[at], out_sem.at[1 + i])
        copy.start()
        outs.append(copy)

    for c in range(CHUNKS):
        for i in range(far_count):
            far_copy(c, i).wait_send()
            mfar_copy(c, i).wait_send()
        for s, (there, _) in enumerate(sides):
            @pl.when(there)
            def _():
                near_copy(c, s).wait_send()
                mnear_copy(c, s).wait_send()
                dec_copy(c, s).wait_send()
    mesh_copy.wait()
    for copy in outs:
        copy.wait()


def body(groups, devs, *args):
    grid_state, mesh_state = args[0], args[1]
    encode_live, encode_far, encode_groups = args[12], args[13], args[14]
    process_far, process_groups, decode_near, decode_live = args[16], args[17], args[18], args[19]
    grid_rows, feats = grid_state.shape
    rows = mesh_state.shape[0]
    width = feats // CHUNKS
    far_count = groups - 1
    long_count = encode_far.shape[0]

    def vmem(*shape, dtype=BF16):
        return pltpu.VMEM(shape, dtype)

    dma = pltpu.SemaphoreType.DMA
    block = (rows, width)
    scratch = [
        vmem(grid_rows, feats), vmem(rows, feats), vmem(9, feats, feats), vmem(3 + long_count, rows, grid_rows),
        pltpu.SMEM(encode_live.shape, jnp.int32), pltpu.SMEM(encode_groups.shape, jnp.int32),
        vmem(3, rows, rows), vmem(*process_far.shape), pltpu.SMEM(process_groups.shape, jnp.int32),
        vmem(*decode_near.shape), pltpu.SMEM(decode_live.shape, jnp.int32),
        vmem(CHUNKS, grid_rows, width),
        vmem(CHUNKS, far_count, *block), vmem(CHUNKS, far_count, *block), vmem(CHUNKS, 2, *block), vmem(CHUNKS, 2, *block),
        vmem(CHUNKS, *block), vmem(CHUNKS, far_count, *block), vmem(CHUNKS, 2, *block),
        vmem(CHUNKS, *block), vmem(CHUNKS, 2, *block),
        vmem(rows, feats), vmem(far_count, rows, rows), vmem(grid_rows, feats, dtype=F32), vmem(rows, feats),
        vmem(grid_rows, feats),
        dma((20,)), dma((CHUNKS, far_count)), dma((CHUNKS, far_count)), dma((CHUNKS, 2)), dma((CHUNKS, 2)),
        dma((CHUNKS, far_count)), dma((CHUNKS, far_count)), dma((CHUNKS, 2)), dma((CHUNKS, 2)),
        dma((CHUNKS, 2)), dma((CHUNKS, 2)), dma((1 + grid_rows // (2 * rows),)),
    ]
    hbm = pl.BlockSpec(memory_space=pl.ANY)
    return pl.pallas_call(
        functools.partial(kernel, groups, devs),
        out_shape=(
            jax.ShapeDtypeStruct(grid_state.shape, BF16),
            jax.ShapeDtypeStruct(mesh_state.shape, BF16),
        ),
        in_specs=[hbm] * len(args),
        out_specs=(hbm, hbm),
        scratch_shapes=scratch,
        compiler_params=pltpu.CompilerParams(collective_id=0, has_side_effects=True),
        name="step",
    )(*args)


def solution(mesh):
    both = ("group", "dev")
    row, whole, second = P(both, None), P(), P(None, both, None)
    flags = P(None, both)
    return jax.shard_map(
        functools.partial(body, mesh.shape["group"], mesh.shape["dev"]),
        mesh=mesh,
        in_specs=(
            row, row, whole, whole, whole, whole, whole, whole, whole, whole, whole,
            second, flags, second, flags, second, second, flags, second, flags,
        ),
        out_specs=(row, row),
        check_vma=False,
    )
```

```python
import functools

import jax
import jax.numpy as jnp
from jax import lax
from jax.experimental import pallas as pl
from jax.experimental.pallas import tpu as pltpu
from jax.sharding import PartitionSpec as P

BF16 = jnp.bfloat16
F32 = jnp.float32
CHUNKS = 2


def silu(x):
    half = 0.5 * x
    return half + half * jnp.tanh(half)


def mm(a, b):
    return jnp.dot(a, b, preferred_element_type=F32)


def layer_norm(v):
    mean = jnp.mean(v, axis=-1, keepdims=True)
    cent = v - mean
    var = jnp.mean(cent * cent, axis=-1, keepdims=True)
    return cent * lax.rsqrt(var + 1e-05)


def partner(me, r, count):
    if count & (count - 1):
        return lax.rem(me + r, count), lax.rem(me + count - r, count)
    out, bit = me, 1
    while bit < count:
        if r & bit:
            out = out + bit * (1 - 2 * lax.rem(me // bit, 2))
        bit *= 2
    return out, out


def kernel(
    groups,
    devs,
    grid_h, mesh_h, ee_h, e1_h, e2_h, pe_h, p1_h, p2_h, de_h, d1_h, d2_h,
    en_h, el_h, ef_h, eg_h, pn_h, pf_h, pg_h, dn_h, dl_h,
    grid_o, mesh_o,
    gs, ms, wt, inc, el, eg, pn, pf, pg, dn, dl,
    em, fheld, fsend, frecv, nsend, nrecv, msend, mfrecv, mnrecv, dsend, dnrecv,
    own_near, proc_inc, dec_own, mesh_out, grid_out,
    load_sem, grid_sem, fs_sem, fr_sem, ns_sem, nr_sem, mfs_sem, mfr_sem, mns_sem, mnr_sem, ds_sem, dr_sem, out_sem,
):
    g = lax.axis_index("group")
    d = lax.axis_index("dev")
    rows, feats = ms.shape
    width = feats // CHUNKS
    far_count = groups - 1
    long_count = pf.shape[0]
    tiles = el.shape[1]
    peers = [partner(g, r, groups) for r in range(1, groups)]
    order = list(reversed(range(far_count)))
    relay = groups == 4
    halves = fsend.shape[1]
    piece_rows = rows // halves
    if relay:
        greeted = [to for to, _ in peers[:2]]
    elif groups & (groups - 1):
        greeted = [to for to, _ in peers] + [source for _, source in peers]
    else:
        greeted = [to for to, _ in peers]
    not_first, not_last = d > 0, d < devs - 1
    sides = ((not_first, d - 1), (not_last, d + 1))

    def load(index, src, dst):
        return pltpu.make_async_copy(src, dst, load_sem.at[index])

    loads = [
        load(0, ee_h, wt.at[0]), load(2, eg_h, eg), load(3, ef_h, inc.at[pl.ds(0, long_count)]),
        load(4, el_h, el), load(5, en_h, inc.at[pl.ds(long_count, 3)]),
        load(6, mesh_h, ms), load(7, e1_h, wt.at[1]), load(8, e2_h, wt.at[2]), load(9, pe_h, wt.at[3]),
        load(10, pg_h, pg), load(11, pn_h, pn), load(12, pf_h, pf), load(13, p1_h, wt.at[4]), load(14, p2_h, wt.at[5]),
        load(15, de_h, wt.at[6]), load(16, dl_h, dl), load(17, dn_h, dn), load(18, d1_h, wt.at[7]), load(19, d2_h, wt.at[8]),
    ]
    step = 2 * rows
    count = gs.shape[0] // step
    grid_loads = [
        pltpu.make_async_copy(grid_h.at[pl.ds(i * step, step)], gs.at[pl.ds(i * step, step)], grid_sem.at[i])
        for i in range(count)
    ]
    loads[0].start()
    for copy in grid_loads:
        copy.start()
    for copy in loads[1:3]:
        copy.start()

    barrier = pltpu.get_barrier_semaphore()
    for to in greeted:
        pl.semaphore_signal(barrier, inc=1, device_id=(to, d), device_id_type=pl.DeviceIdType.MESH)
    for there, near in sides:
        @pl.when(there)
        def _():
            pl.semaphore_signal(barrier, inc=1, device_id=(g, near), device_id_type=pl.DeviceIdType.MESH)

    for side, (there, _) in enumerate(sides):
        @pl.when(jnp.logical_not(there))
        def _():
            for buf in (nrecv, mnrecv, dnrecv):
                for c in range(CHUNKS):
                    buf[c, side] = jnp.zeros((rows, width), BF16)

    def remote(src, dst, send, recv, to):
        return pltpu.make_async_remote_copy(
            src_ref=src, dst_ref=dst, send_sem=send, recv_sem=recv, device_id=to, device_id_type=pl.DeviceIdType.MESH
        )

    def first_axis(h):
        return h % 2

    def far_copy(c, h, i):
        to = i
        if relay:
            to = first_axis(h) if i < 2 else 1 - first_axis(h)
        at = (c, h, i)
        return remote(fsend.at[at], frecv.at[at], fs_sem.at[at], fr_sem.at[at], (peers[to][0], d))

    def near_copy(c, s):
        return remote(nsend.at[c, s], nrecv.at[c, 1 - s], ns_sem.at[c, s], nr_sem.at[c, 1 - s], (g, sides[s][1]))

    def near_in(c, s):
        return remote(nsend.at[c, s], nrecv.at[c, s], ns_sem.at[c, s], nr_sem.at[c, s], (g, sides[s][1]))

    def mfar_copy(c, h, i):
        at = pl.ds(h * piece_rows, piece_rows)
        source, to = msend.at[c, at], i
        if relay and i == 2:
            source, to = mfrecv.at[c, first_axis(h), at], 1 - first_axis(h)
        return remote(source, mfrecv.at[c, i, at], mfs_sem.at[c, h, i], mfr_sem.at[c, h, i], (peers[to][0], d))

    def mnear_copy(c, s):
        return remote(msend.at[c], mnrecv.at[c, 1 - s], mns_sem.at[c, s], mnr_sem.at[c, 1 - s], (g, sides[s][1]))

    def mnear_in(c, s):
        return remote(msend.at[c], mnrecv.at[c, s], mns_sem.at[c, s], mnr_sem.at[c, s], (g, sides[s][1]))

    def dec_copy(c, s):
        return remote(dsend.at[c], dnrecv.at[c, 1 - s], ds_sem.at[c, s], dr_sem.at[c, 1 - s], (g, sides[s][1]))

    def dec_in(c, s):
        return remote(dsend.at[c], dnrecv.at[c, s], ds_sem.at[c, s], dr_sem.at[c, s], (g, sides[s][1]))

    def start_side(copy, c):
        for s, (there, _) in enumerate(sides):
            @pl.when(there)
            def _():
                copy(c, s).start()

    def wait_side(copy, c, s):
        @pl.when(sides[s][0])
        def _():
            copy(c, s).wait_recv()

    loads[0].wait()
    for c in range(CHUNKS):
        cols = pl.ds(c * width, width)
        for i in range(count):
            if c == 0:
                grid_loads[i].wait()
            at = pl.ds(i * step, step)
            em[c, at, :] = silu(mm(gs[at, :], wt[0, :, cols])).astype(BF16)
        if c == 0:
            for copy in loads[3:]:
                copy.start()
            for copy in loads[1:3]:
                copy.wait()
        far = [mm(inc[i], em[c]) for i in range(long_count)]

        def toward(i):
            total = None
            for index in range(long_count):
                flag = jnp.where(eg[0, index] == peers[i][0], 1.0, 0.0).astype(F32)
                term = far[index] * flag
                total = term if total is None else total + term
            return total

        if c == 0:
            pl.semaphore_wait(barrier, len(greeted) + jnp.where(not_first, 1, 0) + jnp.where(not_last, 1, 0))
        if relay:
            totals = [toward(i) for i in range(far_count)]
            for kind in range(2):
                for h in range(halves):
                    at = slice(h * piece_rows, (h + 1) * piece_rows)
                    axis = first_axis(h)
                    fsend[c, h, kind] = totals[2 if kind == 0 else axis][at].astype(BF16)
                    far_copy(c, h, kind).start()
                    if kind == 0:
                        fheld[c, h] = totals[1 - axis][at]
        else:
            for i in order:
                fsend[c, 0, i] = toward(i).astype(BF16)
                far_copy(c, 0, i).start()
        if c == 0:
            for copy in loads[3:5]:
                copy.wait()
            for k in range(3):
                for t in range(tiles):
                    flag = el[k, t].astype(F32).astype(BF16)
                    at = pl.ds(t * rows, rows)
                    inc[long_count + k, :, at] = inc[long_count + k, :, at] * flag
        for s, k in ((0, 0), (1, 2)):
            nsend[c, s] = mm(inc[long_count + k], em[c]).astype(BF16)
        start_side(near_copy, c)
        own_near[:, cols] = mm(inc[long_count + 1], em[c]).astype(BF16)

    if relay:
        for c in range(CHUNKS):
            for h in range(halves):
                far_copy(c, h, 0).wait_recv()
                fsend[c, h, 2] = (fheld[c, h] + frecv[c, h, 0].astype(F32)).astype(BF16)
                far_copy(c, h, 2).start()

    for copy in loads[5:17]:
        copy.wait()
    for i in range(far_count):
        total = None
        for index in range(long_count):
            flag = jnp.where(pg[0, index] == peers[i][1], 1.0, 0.0).astype(F32)
            term = pf[index].astype(F32) * flag
            total = term if total is None else total + term
        proc_inc[i] = total.astype(BF16)
    for k in range(3):
        for t in range(tiles):
            at = pl.ds(t * rows, rows)
            dn[k, at, :] = dn[k, at, :] * dl[k, t].astype(F32).astype(BF16)

    for copy in loads[17:]:
        copy.wait()

    def node_update(residual, summed, first, second):
        hidden = silu(mm(layer_norm(summed).astype(BF16), wt[first])).astype(BF16)
        return (residual.astype(F32) + mm(hidden, wt[second])).astype(BF16)

    parts = []
    for c in range(CHUNKS):
        total = own_near[:, pl.ds(c * width, width)].astype(F32)
        for s in range(2):
            wait_side(near_in, c, s)
            total = total + nrecv[c, s].astype(F32)
        pieces = []
        for h in range(halves):
            piece = total[h * piece_rows:(h + 1) * piece_rows]
            for i in (1, 2) if relay else order:
                far_copy(c, h, i).wait_recv()
                piece = piece + frecv[c, h, i].astype(F32)
            pieces.append(piece)
        parts.append(jnp.concatenate(pieces, axis=0))
    mesh_mid = node_update(ms[...], jnp.concatenate(parts, axis=1), 1, 2)

    for c in range(CHUNKS):
        msend[c] = silu(mm(mesh_mid, wt[3, :, pl.ds(c * width, width)])).astype(BF16)
        if not relay:
            for i in order:
                mfar_copy(c, 0, i).start()
        else:
            for h in range(halves):
                mfar_copy(c, h, first_axis(h)).start()
        start_side(mnear_copy, c)
    if relay:
        for c in range(CHUNKS):
            for h in range(halves):
                mfar_copy(c, h, 1 - first_axis(h)).start()
    parts = [mm(pn[1], msend[c]) for c in range(CHUNKS)]
    if relay:
        for c in range(CHUNKS):
            for h in range(halves):
                mfar_copy(c, h, first_axis(h)).wait_recv()
                mfar_copy(c, h, 2).start()
    for c in range(CHUNKS):
        for s in range(2):
            wait_side(mnear_in, c, s)
            parts[c] = parts[c] + mm(pn[2 * s], mnrecv[c, s])
    for i in range(far_count) if relay else order:
        for c in range(CHUNKS):
            for h in range(halves):
                if not relay or i != first_axis(h):
                    mfar_copy(c, h, i).wait_recv()
            parts[c] = parts[c] + mm(proc_inc[i], mfrecv[c, i])
    mesh_next = node_update(mesh_mid, jnp.concatenate(parts, axis=1), 4, 5)
    mesh_out[...] = mesh_next

    for c in range(CHUNKS):
        dsend[c] = silu(mm(mesh_next, wt[6, :, pl.ds(c * width, width)])).astype(BF16)
        start_side(dec_copy, c)
    mesh_copy = pltpu.make_async_copy(mesh_out, mesh_o, out_sem.at[0])
    mesh_copy.start()

    def own_part(i, carry):
        at = pl.ds(pl.multiple_of(i * step, step), step)
        for c in range(CHUNKS):
            dec_own[at, pl.ds(c * width, width)] = mm(dn[1, at, :], dsend[c])
        return carry

    lax.fori_loop(0, count, own_part, 0)
    for c in range(CHUNKS):
        for s in range(2):
            wait_side(dec_in, c, s)
    outs = []
    for i in range(count):
        at = pl.ds(i * step, step)
        sums = []
        for c in range(CHUNKS):
            total = dec_own[at, pl.ds(c * width, width)]
            for s in range(2):
                total = total + mm(dn[2 * s, at, :], dnrecv[c, s])
            sums.append(total)
        grid_out[at, :] = node_update(gs[at, :], jnp.concatenate(sums, axis=1), 7, 8)
        copy = pltpu.make_async_copy(grid_out.at[at], grid_o.at[at], out_sem.at[1 + i])
        copy.start()
        outs.append(copy)

    for c in range(CHUNKS):
        for i in range(far_count):
            for h in range(halves):
                far_copy(c, h, i).wait_send()
                mfar_copy(c, h, i).wait_send()
        for s, (there, _) in enumerate(sides):
            @pl.when(there)
            def _():
                near_copy(c, s).wait_send()
                mnear_copy(c, s).wait_send()
                dec_copy(c, s).wait_send()
    mesh_copy.wait()
    for copy in outs:
        copy.wait()


def body(groups, devs, *args):
    grid_state, mesh_state = args[0], args[1]
    args = list(args)
    args[14], args[17] = args[14].T, args[17].T
    encode_live, encode_far, encode_groups = args[12], args[13], args[14]
    process_far, process_groups, decode_near, decode_live = args[16], args[17], args[18], args[19]
    grid_rows, feats = grid_state.shape
    rows = mesh_state.shape[0]
    width = feats // CHUNKS
    far_count = groups - 1
    long_count = encode_far.shape[0]

    def vmem(*shape, dtype=BF16):
        return pltpu.VMEM(shape, dtype)

    dma = pltpu.SemaphoreType.DMA
    halves = 2 if groups == 4 else 1
    pieces = (CHUNKS, halves, far_count)
    piece = (rows // halves, width)
    block = (rows, width)
    scratch = [
        vmem(grid_rows, feats), vmem(rows, feats), vmem(9, feats, feats), vmem(3 + long_count, rows, grid_rows),
        pltpu.SMEM(encode_live.shape, jnp.int32), pltpu.SMEM(encode_groups.shape, jnp.int32),
        vmem(3, rows, rows), vmem(*process_far.shape), pltpu.SMEM(process_groups.shape, jnp.int32),
        vmem(*decode_near.shape), pltpu.SMEM(decode_live.shape, jnp.int32),
        vmem(CHUNKS, grid_rows, width),
        vmem(CHUNKS, halves, *piece, dtype=F32), vmem(*pieces, *piece), vmem(*pieces, *piece),
        vmem(CHUNKS, 2, *block), vmem(CHUNKS, 2, *block),
        vmem(CHUNKS, *block), vmem(CHUNKS, far_count, *block), vmem(CHUNKS, 2, *block),
        vmem(CHUNKS, *block), vmem(CHUNKS, 2, *block),
        vmem(rows, feats), vmem(far_count, rows, rows), vmem(grid_rows, feats, dtype=F32), vmem(rows, feats),
        vmem(grid_rows, feats),
        dma((20,)), dma((grid_rows // (2 * rows),)), dma(pieces), dma(pieces), dma((CHUNKS, 2)), dma((CHUNKS, 2)),
        dma(pieces), dma(pieces), dma((CHUNKS, 2)), dma((CHUNKS, 2)),
        dma((CHUNKS, 2)), dma((CHUNKS, 2)), dma((1 + grid_rows // (2 * rows),)),
    ]
    hbm = pl.BlockSpec(memory_space=pl.ANY)
    return pl.pallas_call(
        functools.partial(kernel, groups, devs),
        out_shape=(
            jax.ShapeDtypeStruct(grid_state.shape, BF16),
            jax.ShapeDtypeStruct(mesh_state.shape, BF16),
        ),
        in_specs=[hbm] * len(args),
        out_specs=(hbm, hbm),
        scratch_shapes=scratch,
        compiler_params=pltpu.CompilerParams(collective_id=0, has_side_effects=True),
        name="step",
    )(*args)


def solution(mesh):
    both = ("group", "dev")
    row, whole, second = P(both, None), P(), P(None, both, None)
    flags = P(None, both)
    return jax.shard_map(
        functools.partial(body, mesh.shape["group"], mesh.shape["dev"]),
        mesh=mesh,
        in_specs=(
            row, row, whole, whole, whole, whole, whole, whole, whole, whole, whole,
            second, flags, second, flags, second, second, flags, second, flags,
        ),
        out_specs=(row, row),
        check_vma=False,
    )
```
